16 devices in a mesh: dp: 4 (over y, z, core), tp: 4 (over x).
Axes of the slice: x: 4, y: 2, z: 1, core: 2. Of those that a mesh axis runs over, the one named last changes fastest.
The devices are a block of a 4x4x8 slice.
Arguments:
- x: bfloat16 [4, 1024, 4096], P('dp', 'tp'), parts along dimension 0
- dy: bfloat16 [4, 1024, 4096], P('dp', 'tp'), parts along dimension 0
- wq: bfloat16 [4096, 4096], P(None, 'tp')
- wk: bfloat16 [4096, 1024], P(None, 'tp')
- wv: bfloat16 [4096, 1024], P(None, 'tp')
- wo: bfloat16 [4096, 4096], P('tp')
- w_gate: bfloat16 [4096, 12800], P(None, 'tp')
- w_up: bfloat16 [4096, 12800], P(None, 'tp')
- w_down: bfloat16 [12800, 4096], P('tp')
Outputs:
- output 1: bfloat16 [4, 1024, 4096], P('dp', 'tp'), parts along dimension 0
- output 2: bfloat16 [16384, 4096], P('dp', 'tp'), parts along dimension 0
- output 3: bfloat16 [16384, 1024], P('dp', 'tp'), parts along dimension 0
- output 4: bfloat16 [16384, 1024], P('dp', 'tp'), parts along dimension 0
- output 5: bfloat16 [16384, 4096], P(('dp', 'tp')), parts along dimension 0
- output 6: bfloat16 [16384, 12800], P('dp', 'tp'), parts along dimension 0
- output 7: bfloat16 [16384, 12800], P('dp', 'tp'), parts along dimension 0
- output 8: bfloat16 [51200, 4096], P(('dp', 'tp')), parts along dimension 0
There are 4 independent parts. The reference program is written for one: setup_inputs(seed, part) draws one part's arguments, and reference() takes and returns one part's arrays. A program takes and returns all parts, laid end to end along the dimension named above; an argument that names none is the same for every part.
All inputs are finite; a program needn't handle non-finite values.
Results may differ from the reference program's by a relative error of at most 0.024.
Values are sent between devices in bfloat16 or wider.
A program may use at most 768 MiB of HBM per device.

```python
import jax
import jax.numpy as jnp
from jax import lax

SEQUENCES = 1
TOKENS = 1024
D = 4096
HEADS = 32
KV_HEADS = 8
HEAD = 128
FF = 12800
THETA = 10000
NAMES = ("wq", "wk", "wv", "wo", "w_gate", "w_up", "w_down")
SHAPES = {
    "wq": (D, HEADS * HEAD),
    "wk": (D, KV_HEADS * HEAD),
    "wv": (D, KV_HEADS * HEAD),
    "wo": (HEADS * HEAD, D),
    "w_gate": (D, FF),
    "w_up": (D, FF),
    "w_down": (FF, D),
}


def bump(key, n, height):
    away = (jnp.arange(n, dtype=jnp.int32) - jax.random.randint(key, (), 0, n, jnp.int32)) % n
    return jnp.where(away < n // 8, height, 1.0)


def together(key, own, strength):
    shared = jax.random.normal(key, own.shape[1:], jnp.float32)
    return (own + strength * shared) * lax.rsqrt(1 + strength * strength)


def setup_inputs(seed: int = 0, part: int = 0) -> dict:
    kx, kdy, ka, kb, kz, kf, kh, kl, *kw = jax.random.split(jax.random.key(seed), 8 + len(NAMES))
    kx, kdy, ka, kb = (jax.random.fold_in(k, part) for k in (kx, kdy, ka, kb))
    shape = (SEQUENCES, TOKENS, D)
    much_x, much_dy = jax.random.uniform(kz, (2,), jnp.float32, 0.0, 1.0)
    loud = 2.0 ** jax.random.uniform(jax.random.fold_in(kz, 1), (), jnp.float32, -1.0, 2.0)
    halves = 2.0 ** jax.random.uniform(kl, (2,), jnp.float32, -1.0, 1.0)
    times = {"wq": 1.0, "wk": 1.0, "wv": 2.0, "wo": halves[0], "w_gate": 1.0, "w_up": bump(kh, FF, 4.0), "w_down": halves[1]}
    x = together(ka, jax.random.normal(kx, shape, jnp.float32), much_x) * bump(kf, D, 4.0)
    dy = together(kb, jax.random.normal(kdy, shape, jnp.float32), much_dy)
    drawn = {"x": x.astype(jnp.bfloat16), "dy": (loud * dy * (SEQUENCES * TOKENS) ** -0.5).astype(jnp.bfloat16)}
    for key, name in zip(kw, NAMES, strict=True):
        drawn[name] = (jax.random.normal(key, SHAPES[name], jnp.float32) * SHAPES[name][0] ** -0.5 * times[name]).astype(jnp.bfloat16)
    return drawn


def matmul(a, w):
    return jnp.dot(a, w, preferred_element_type=jnp.float32).astype(jnp.bfloat16)


def normed(h):
    wide = h.astype(jnp.float32)
    scale = lax.rsqrt(jnp.mean(wide**2, -1, keepdims=True) + 1e-6)
    return (wide * scale).astype(jnp.bfloat16)


def turned(t, theta):
    half = t.shape[-1] // 2
    angle = jnp.arange(t.shape[0], dtype=jnp.float32)[:, None] * theta ** (-jnp.arange(half, dtype=jnp.float32) / half)
    cos, sin = jnp.cos(angle)[:, None], jnp.sin(angle)[:, None]
    a, b = t[..., :half].astype(jnp.float32), t[..., half:].astype(jnp.float32)
    return jnp.concatenate([a * cos - b * sin, b * cos + a * sin], -1).astype(jnp.bfloat16)


def seen_by(q, k, v):
    tokens, kv = q.shape[0], k.shape[1]
    q = q.reshape(tokens, kv, -1, q.shape[-1])
    scores = jnp.einsum("tgsd,ugd->gstu", q.astype(jnp.float32), k.astype(jnp.float32)) * q.shape[-1] ** -0.5
    place = jnp.arange(tokens)
    weights = jax.nn.softmax(jnp.where(place[:, None] >= place, scores, -jnp.inf), -1).astype(jnp.bfloat16)
    return jnp.einsum("gstu,ugd->tgsd", weights.astype(jnp.float32), v.astype(jnp.float32)).astype(jnp.bfloat16).reshape(tokens, -1)


def layer(h, w):
    a = normed(h)
    q, k = (turned(matmul(a, w[name]).reshape(h.shape[0], -1, HEAD), THETA) for name in ("wq", "wk"))
    h = h + matmul(seen_by(q, k, matmul(a, w["wv"]).reshape(h.shape[0], -1, HEAD)), w["wo"])
    b = normed(h)
    gate = jnp.dot(b, w["w_gate"], preferred_element_type=jnp.float32)
    up = jnp.dot(b, w["w_up"], preferred_element_type=jnp.float32)
    return h + matmul((jax.nn.silu(gate) * up).astype(jnp.bfloat16), w["w_down"])


def reference(x, dy, wq, wk, wv, wo, w_gate, w_up, w_down):
    weights = dict(zip(NAMES, (wq, wk, wv, wo, w_gate, w_up, w_down), strict=True))

    def take(so_far, sequence):
        h, by_y = sequence
        _, back = jax.vjp(lambda w, h: layer(h, w), weights, h)
        by_weights, by_h = back(by_y)
        return jax.tree.map(lambda total, term: total + term.astype(jnp.float32), so_far, by_weights), by_h

    none_yet = {name: jnp.zeros(w.shape, jnp.float32) for name, w in weights.items()}
    by_weights, by_x = lax.scan(take, none_yet, (x, dy))
    return (by_x, *(by_weights[name].astype(jnp.bfloat16) for name in NAMES))
```

```python
import functools

import jax
import jax.numpy as jnp
from jax import lax
from jax.experimental import pallas as pl
from jax.experimental.pallas import tpu as pltpu
from jax.sharding import PartitionSpec as P

HEAD = 128
THETA = 10000
HIDDEN = -2e30
LOG2E = 1.4426950408889634
VMEM = 56 * 2**20
STRIP = 512


def _dot(a, b, ca=1, cb=0):
    return lax.dot_general(a, b, (((ca,), (cb,)), ((), ())), preferred_element_type=jnp.float32)


def bf(t):
    return t.astype(jnp.bfloat16)


def call(body, grid, ins, outs, scratch, args, flops, exps=0, aliases={}):
    shapes = [jax.ShapeDtypeStruct(shape, dtype) for shape, dtype, _ in outs]
    moved = sum(t.size * t.dtype.itemsize for t in (*args, *shapes))
    return pl.pallas_call(
        body, grid=grid, in_specs=ins, out_specs=[spec for _, _, spec in outs], out_shape=shapes, scratch_shapes=scratch,
        input_output_aliases=aliases, compiler_params=pltpu.CompilerParams(dimension_semantics=("arbitrary",) * len(grid), vmem_limit_bytes=VMEM),
        cost_estimate=pl.CostEstimate(flops=flops, transcendentals=exps, bytes_accessed=moved),
    )(*args)


def _strip(ref, i, at, wide, bq, g):
    if wide <= bq:
        head = i * g + at // bq
        return ref[at % bq : at % bq + wide, head * HEAD : (head + 1) * HEAD]
    return jnp.concatenate([ref[:, h * HEAD : (h + 1) * HEAD] for h in range(i * g + at // bq, i * g + (at + wide) // bq)], axis=0)


def _gap(bk, cols, bq):
    return lax.rem(lax.broadcasted_iota(jnp.int32, (bk, cols), 1), bq) - lax.broadcasted_iota(jnp.int32, (bk, cols), 0)


def _look(q_ref, k_ref, v_ref, o_ref, lse_ref, top_s, mix_s, gap_s, *, g, bk, scale):
    bq, kv = q_ref.shape[0], k_ref.shape[1] // HEAD
    cols = g * bq
    iq = pl.program_id(0)
    e = scale * LOG2E
    wide = min(cols, STRIP)
    pieces = [(i, at) for i in range(kv) for at in range(0, cols, wide)]

    @pl.when(iq == 0)
    def _():
        gap_s[...] = _gap(bk, cols, bq)

    top_s[...] = jnp.full(top_s.shape, -1e30, jnp.float32)
    mix_s[...] = jnp.zeros_like(mix_s)
    ones = jnp.ones((8, bk), q_ref.dtype)

    def block(j, masked):
        here = pl.ds(pl.multiple_of(j * bk, bk), bk)
        scores = [_dot(k_ref[here, i * HEAD : (i + 1) * HEAD], _strip(q_ref, i, at, wide, bq, g), 1, 1) for i, at in pieces]
        ok = gap_s[...] >= j * bk - iq * bq if masked else None
        weights, keeps = [], []
        for (i, at), s in zip(pieces, scores):
            if masked:
                s = jnp.where(ok[:, at : at + wide], s, HIDDEN)
            old = top_s[i : i + 1, at : at + wide]
            top = jnp.maximum(old, s.max(axis=0, keepdims=True))
            top_s[i : i + 1, at : at + wide] = top
            weights.append(bf(jnp.exp2((s - top) * e)))
            keeps.append(jnp.exp2((old - top) * e))
        for (i, at), p, keep in zip(pieces, weights, keeps):
            values = jnp.concatenate([v_ref[here, i * HEAD : (i + 1) * HEAD].T, ones], axis=0)
            mix_s[i, :, at : at + wide] = mix_s[i, :, at : at + wide] * keep + _dot(values, p)

    whole = iq * bq // bk
    lax.fori_loop(0, whole, lambda j, _: block(j, False), None)
    lax.fori_loop(whole, whole + bq // bk, lambda j, _: block(j, True), None)
    for i in range(kv):
        total = mix_s[i, HEAD : HEAD + 1, :]
        out = (mix_s[i, :HEAD, :] * (1 / total)).T
        lse = top_s[i : i + 1, :] * scale + jnp.log(total)
        for m in range(g):
            o_ref[:, (i * g + m) * HEAD : (i * g + m + 1) * HEAD] = bf(out[m * bq : (m + 1) * bq])
            lse_ref[i, m : m + 1, :] = lse[:, m * bq : (m + 1) * bq]


def look(qkv, h, kv, bq=512, bk=256):
    t, g = qkv.shape[0], h // kv
    return call(
        functools.partial(_look, g=g, bk=bk, scale=HEAD**-0.5), (t // bq,),
        [pl.BlockSpec((bq, h * HEAD), lambda i: (i, 0)), pl.BlockSpec((t, kv * HEAD), lambda i: (0, g)), pl.BlockSpec((t, kv * HEAD), lambda i: (0, g + 1))],
        [((t, h * HEAD), jnp.bfloat16, pl.BlockSpec((bq, h * HEAD), lambda i: (i, 0))),
         ((kv, g, t), jnp.float32, pl.BlockSpec((kv, g, bq), lambda i: (0, 0, i)))],
        [pltpu.VMEM((kv, g * bq), jnp.float32), pltpu.VMEM((kv, HEAD + 8, g * bq), jnp.float32), pltpu.VMEM((bk, g * bq), jnp.int32)],
        (qkv, qkv, qkv), 4 * h * t * t * HEAD, h * t * t)


def _look_back(*refs, g, bk, scale, stream, parts):
    q_ref, k_ref, v_ref, do_ref, o_ref, lse_ref, cos_q, sin_q, *rest = refs
    if stream > 0:
        dk_in, dv_in, *rest = rest
    if stream == parts - 1:
        cos_k, sin_k, dq_ref, dkv_ref, *rest = rest
    else:
        dq_ref, dk_out, dv_out, *rest = rest
    dq_s, dk_s, dv_s, delta_s, gap_s = rest
    q, o = (ref.at[0, 0] for ref in (q_ref, o_ref))
    bq, kv = do_ref.shape[0], k_ref.shape[1] // HEAD
    cols = g * bq
    iq = pl.program_id(0)
    start = (iq * parts + stream) * bq
    e = scale * LOG2E
    wide = min(cols, STRIP)
    pieces = [(i, at) for i in range(kv) for at in range(0, cols, wide)]
    half = HEAD // 2

    @pl.when(iq == 0)
    def _():
        gap_s[...] = _gap(bk, cols, bq)
        dk_s[...] = dk_in[...] if stream > 0 else jnp.zeros_like(dk_s)
        dv_s[...] = dv_in[...] if stream > 0 else jnp.zeros_like(dv_s)

    dq_s[...] = jnp.zeros_like(dq_s)
    for i, at in pieces:
        both = _strip(do_ref, i, at, wide, bq, g).astype(jnp.float32) * _strip(o, i, at, wide, bq, g).astype(jnp.float32)
        delta_s[i : i + 1, at : at + wide] = both.T.sum(axis=0, keepdims=True)
    lses = [jnp.concatenate([lse_ref[i, m : m + 1, :] for m in range(g)], axis=1) * LOG2E for i in range(kv)]

    def block(j, masked):
        here = pl.ds(pl.multiple_of(j * bk, bk), bk)
        qs = [_strip(q, i, at, wide, bq, g) for i, at in pieces]
        dos = [_strip(do_ref, i, at, wide, bq, g) for i, at in pieces]
        keys = [k_ref[here, i * HEAD : (i + 1) * HEAD] for i in range(kv)]
        values = [v_ref[here, i * HEAD : (i + 1) * HEAD] for i in range(kv)]
        scores = [_dot(keys[i], x, 1, 1) for (i, _), x in zip(pieces, qs)]
        dps = [_dot(values[i], x, 1, 1) for (i, _), x in zip(pieces, dos)]
        ok = gap_s[...] >= j * bk - start if masked else None
        for m, (i, at) in enumerate(pieces):
            p = jnp.exp2(scores[m] * e - lses[i][:, at : at + wide])
            if masked:
                p = jnp.where(ok[:, at : at + wide], p, 0.0)
            ds = bf(p * (dps[m] - delta_s[i : i + 1, at : at + wide]))
            dv_s[i, here, :] += _dot(bf(p), dos[m])
            dk_s[i, here, :] += _dot(ds, qs[m])
            dq_s[i, :, at : at + wide] += _dot(keys[i].T, ds)

    whole, last = start // bk, (start + bq + bk - 1) // bk
    lax.fori_loop(0, whole, lambda j, _: block(j, False), None)
    lax.fori_loop(whole, last, lambda j, _: block(j, True), None)
    cos, sin = (jnp.concatenate([ref[...]] * g, axis=1) for ref in (cos_q, sin_q))
    for i in range(kv):
        dq = dq_s[i] * scale
        a, b = dq[:half], dq[half:]
        dq = jnp.concatenate([a * cos + b * sin, b * cos - a * sin], axis=0).T
        for m in range(g):
            dq_ref[:, (i * g + m) * HEAD : (i * g + m + 1) * HEAD] = bf(dq[m * bq : (m + 1) * bq])

    @pl.when(iq == pl.num_programs(0) - 1)
    def _():
        if stream < parts - 1:
            dk_out[...] = dk_s[...]
            dv_out[...] = dv_s[...]
            return
        for i in range(kv):
            dk = dk_s[i] * scale
            dkv_ref[:, i * HEAD : (i + 1) * HEAD] = bf(dk * cos_k[...] - pltpu.roll(dk, half, 1) * sin_k[...])
            dkv_ref[:, (kv + i) * HEAD : (kv + i + 1) * HEAD] = bf(dv_s[i])


def look_back(stream, parts, n, qkv, h, kv, d_out, out, lse, cos, sin, sums=(), bk=256):
    t, g = qkv.shape[0], h // kv
    half, bq = HEAD // 2, d_out.shape[0] // n
    view = lambda x: x.reshape(n, parts, bq, x.shape[-1])
    rows = pl.BlockSpec((1, 1, bq, h * HEAD), lambda i: (i, stream, 0, 0))
    tall = pl.BlockSpec((half, bq), lambda i: (0, i * parts + stream))
    flat = pl.BlockSpec((t, HEAD), lambda i: (0, 0))
    sum_ = pl.BlockSpec((kv, t, HEAD), lambda i: (0, 0, 0))
    mine = pl.BlockSpec((bq, h * HEAD), lambda i: (i, 0))
    ends = stream == parts - 1
    outs = [((n * bq, h * HEAD), jnp.bfloat16, mine)]
    outs += [((t, 2 * kv * HEAD), jnp.bfloat16, pl.BlockSpec((t, 2 * kv * HEAD), lambda i: (0, 0)))] if ends else [((kv, t, HEAD), jnp.float32, sum_)] * 2
    return call(
        functools.partial(_look_back, g=g, bk=bk, scale=HEAD**-0.5, stream=stream, parts=parts), (n,),
        [rows, pl.BlockSpec((t, kv * HEAD), lambda i: (0, g)), pl.BlockSpec((t, kv * HEAD), lambda i: (0, g + 1)), mine, rows,
         pl.BlockSpec((kv, g, bq), lambda i: (0, 0, i * parts + stream)), tall, tall] + [sum_] * len(sums) + [flat] * (2 * ends),
        outs,
        [pltpu.VMEM((kv, HEAD, g * bq), jnp.float32), pltpu.VMEM((kv, t, HEAD), jnp.float32), pltpu.VMEM((kv, t, HEAD), jnp.float32),
         pltpu.VMEM((kv, g * bq), jnp.float32), pltpu.VMEM((bk, g * bq), jnp.int32)],
        (view(qkv), qkv, qkv, d_out, view(out), lse, cos[:, :half].T, sin[:, half:].T, *sums, *((cos, sin) if ends else ())),
        10 * h * t * n * bq * HEAD, h * t * n * bq)


def _first(x_ref, cos_ref, sin_ref, wq_ref, wk_ref, wv_ref, a_ref, w_ref, out_ref, got_s, w_s, sent, got, own, *, n, turned):
    me = lax.axis_index("tp")
    left, right, across = (lax.rem(me + i, n) for i in (n - 1, 1, 2))
    tokens = x_ref.shape[0]
    h = tokens // 2
    wide = 4 * HEAD
    top, bottom = pl.ds(0, h), pl.ds(h, h)

    barrier = pltpu.get_barrier_semaphore()
    for device in (left, right):
        pl.semaphore_signal(barrier, inc=1, device_id={"tp": device}, device_id_type=pl.DeviceIdType.MESH)
    pl.semaphore_wait(barrier, 2)

    def send(k, part, slot, rows, device):
        copy = pltpu.make_async_remote_copy(src_ref=part, dst_ref=got_s.at[slot, rows], send_sem=sent.at[k], recv_sem=got.at[k],
                                            device_id={"tp": device}, device_id_type=pl.DeviceIdType.MESH)
        copy.start()
        return copy

    copies = [send(0, x_ref.at[top], 0, top, right), send(1, x_ref.at[bottom], 0, bottom, left),
              send(2, x_ref.at[bottom], 1, top, right), send(3, x_ref.at[top], 1, bottom, left)]
    local = []

    def move(part, to):
        copy = pltpu.make_async_copy(part, to, own.at[len(local)])
        copy.start()
        local.append(copy)

    at = 0
    for ref in (wq_ref, wk_ref, wv_ref):
        move(ref, w_s.at[:, pl.ds(at, ref.shape[1])])
        at += ref.shape[1]
    for copy in local:
        copy.wait()
    waited = len(local)
    move(w_s, w_ref)

    def keep(part, starts):
        size = tokens // len(starts)
        starts = [pl.multiple_of(start, size) for start in starts]
        for i, start in enumerate(starts):
            move(part.at[pl.ds(i * size, size)], a_ref.at[pl.ds(start, size)])

        def columns(t, _):
            y = _dot(part[...], w_s[:, pl.ds(pl.multiple_of(t * wide, wide), wide)])
            for i, start in enumerate(starts):
                here = pl.ds(start, size)
                for m in range(wide // HEAD):
                    x = bf(y[i * size : (i + 1) * size, m * HEAD : (m + 1) * HEAD]).astype(jnp.float32)
                    z = x * cos_ref[here, :] + pltpu.roll(x, HEAD // 2, 1) * sin_ref[here, :]
                    z = jnp.where(t * (wide // HEAD) + m < turned, z, x)
                    out_ref[here, pl.ds(pl.multiple_of(t * wide + m * HEAD, HEAD), HEAD)] = bf(z)

        lax.fori_loop(0, w_s.shape[1] // wide, columns, None)

    keep(x_ref, [me * tokens])
    for copy in copies[:2]:
        copy.wait_recv()
    copies += [send(4, got_s.at[0, top], 2, top, right), send(5, got_s.at[0, bottom], 2, bottom, left)]
    keep(got_s.at[0], [left * tokens, right * tokens + h])
    for copy in copies[2:4]:
        copy.wait_recv()
    keep(got_s.at[1], [left * tokens + h, right * tokens])
    for copy in copies[4:]:
        copy.wait_recv()
    keep(got_s.at[2], [across * tokens])
    for copy in copies:
        copy.wait_send()
    for copy in local[waited:]:
        copy.wait()


def first(x, wq, wk, wv, cos, sin, n):
    tokens, d = x.shape
    c = wq.shape[1] + wk.shape[1] + wv.shape[1]
    anywhere, vmem = pl.BlockSpec(memory_space=pl.ANY), pl.BlockSpec(memory_space=pltpu.VMEM)
    return pl.pallas_call(
        functools.partial(_first, n=n, turned=(wq.shape[1] + wk.shape[1]) // HEAD),
        in_specs=[vmem] * 3 + [anywhere] * 3, out_specs=[anywhere, anywhere, vmem],
        out_shape=[jax.ShapeDtypeStruct(shape, x.dtype) for shape in ((n * tokens, d), (d, c), (n * tokens, c))],
        scratch_shapes=[pltpu.VMEM((n - 1, tokens, d), x.dtype), pltpu.VMEM((d, c), x.dtype), pltpu.SemaphoreType.DMA((6,)),
                        pltpu.SemaphoreType.DMA((6,)), pltpu.SemaphoreType.DMA((10,))],
        compiler_params=pltpu.CompilerParams(collective_id=0, has_side_effects=True, vmem_limit_bytes=VMEM),
        cost_estimate=pl.CostEstimate(flops=2 * n * tokens * d * c, transcendentals=0, bytes_accessed=2 * (2 * n * tokens * d + 2 * d * c + n * tokens * c)),
    )(x, cos, sin, wq, wk, wv)


def plain(t, column=0):
    return t, t.shape[:-1], (0,) * (t.ndim - 1), column


def _mlp(b_ref, d_ref, wg_ref, wu_ref, hidden_ref, dg_ref, du_ref, turned_ref, *, last):
    b = b_ref[...]
    gate, up = _dot(b, wg_ref[...]), _dot(b, wu_ref[...])
    d = d_ref[...].reshape(gate.shape).astype(jnp.float32)
    s = jax.nn.sigmoid(gate)
    act = gate * s
    hidden_ref[...] = bf(act * up).T
    du_ref[...] = bf(d * act)
    dg_ref[...] = bf(d * up * (s * (1 + gate * (1 - s))))
    rows = turned_ref.shape[0]
    turned_ref[...] = b_ref[:, pl.ds(pl.multiple_of(jnp.minimum(pl.program_id(0), last) * rows, rows), rows)].T


def mlp(b, d_hidden, w_gate, w_up, wide=256, rows=512):
    tokens, d = b.shape
    units = w_gate.shape[1]
    columns = pl.BlockSpec((d, wide), lambda j: (0, j))
    t, lead, index, _ = d_hidden
    out = ((tokens, units), jnp.bfloat16, pl.BlockSpec((tokens, wide), lambda j: (0, j)))
    last = d // rows - 1
    return call(functools.partial(_mlp, last=last), (pl.cdiv(units, wide),),
                [pl.BlockSpec((tokens, d), lambda j: (0, 0)), pl.BlockSpec((*lead, wide), lambda j: (*index, j)), columns, columns],
                [((units, tokens), jnp.bfloat16, pl.BlockSpec((wide, tokens), lambda j: (j, 0))), out, out,
                 ((d, tokens), jnp.bfloat16, pl.BlockSpec((rows, tokens), lambda j: (jnp.minimum(j, last), 0)))],
                [], (b, t, w_gate, w_up), 4 * tokens * d * units, tokens * units)


def _mlp_back(dg_ref, du_ref, wg_ref, wu_ref, o_ref):
    o_ref[...] = bf(_dot(dg_ref[...], wg_ref[...], 1, 1) + _dot(du_ref[...], wu_ref[...], 1, 1))


def mlp_back(d_gate, d_up, w_gate, w_up, wide=512):
    tokens, units = d_gate.shape
    d = w_gate.shape[0]
    whole = pl.BlockSpec((tokens, units), lambda j: (0, 0))
    rows = pl.BlockSpec((wide, units), lambda j: (j, 0))
    return call(_mlp_back, (d // wide,), [whole, whole, rows, rows], [((tokens, d), jnp.bfloat16, pl.BlockSpec((tokens, wide), lambda j: (0, j)))], [],
                (d_gate, d_up, w_gate, w_up), 4 * tokens * d * units)[0]


def _back(x_ref, w_ref, o_ref):
    o_ref[...] = bf(_dot(x_ref[...], w_ref[...], 1, 1))


def back(x, w, wide):
    m, k = x.shape
    return call(_back, (w.shape[0] // wide,), [pl.BlockSpec((m, k), lambda j: (0, 0)), pl.BlockSpec((wide, k), lambda j: (j, 0))],
                [((m, w.shape[0]), jnp.bfloat16, pl.BlockSpec((m, wide), lambda j: (0, j)))], [], (x, w), 2 * m * k * w.shape[0])[0]


def _qkv_back(*refs):
    *dq_refs, dkv_ref, w_ref, o_ref = refs
    for s, ref in enumerate(dq_refs):
        dkv = dkv_ref[:, s].reshape(ref.shape[0], -1)
        o_ref[:, s] = bf(_dot(jnp.concatenate([ref[...], dkv], axis=1), w_ref[...], 1, 1)).reshape(o_ref.shape[0], *o_ref.shape[2:])


def qkv_back(dqs, dkv, w, n, wide=512):
    parts, (tokens, c), d = len(dqs), dqs[0].shape, w.shape[0]
    size = tokens // n
    view = lambda w_: ((n, parts, size, w_), lambda j: (0, 0, 0, 0))
    return call(_qkv_back, (d // wide,), [pl.BlockSpec((tokens, c), lambda j: (0, 0))] * parts + [pl.BlockSpec(*view(dkv.shape[1])), pl.BlockSpec((wide, w.shape[1]), lambda j: (j, 0))],
                [((n, parts, size, d), jnp.bfloat16, pl.BlockSpec((n, parts, size, wide), lambda j: (0, 0, 0, j)))], [],
                (*dqs, dkv.reshape(n, parts, size, -1), w), 2 * parts * tokens * w.shape[1] * d)[0].reshape(parts * tokens, d)


def _outer(*refs, parts, outs, begun, turned):
    refs = refs[begun:]
    a, b, out, turned_s = refs[:parts], refs[parts : parts * (1 + outs)], refs[parts * (1 + outs) : -1], refs[-1]

    @pl.when(pl.program_id(1) == 0)
    def _():
        at = 0
        for ref in a:
            x = ref[...] if turned else ref[...].reshape(-1, ref.shape[-1]).T
            turned_s[:, at : at + x.shape[1]] = x
            at += x.shape[1]

    for i in range(outs):
        right = [b[i * parts + m][...].reshape(-1, out[i].shape[-1]) for m in range(parts)]
        out[i][...] = bf(_dot(turned_s[...], jnp.concatenate(right, axis=0) if parts > 1 else right[0]))


def outer(a, bs, rows, steps, wides, span=None, begun=None, turned=False):
    parts, m = len(a), a[0][0].shape[0 if turned else -1]
    size = lambda lead: functools.reduce(lambda x, y: x * y, lead, 1)
    depth = sum(t.shape[1] if turned else size(lead) for t, lead, _, _ in a)
    begin, end = span or (0, m // rows)
    begun = begun or []
    ins = [pl.BlockSpec(memory_space=pl.ANY) for _ in begun]
    if turned:
        ins += [pl.BlockSpec((rows, t.shape[1]), lambda i, j: (i + begin, 0)) for t, *_ in a]
    else:
        ins += [pl.BlockSpec((*lead, rows), lambda i, j, index=index: (*index, i + begin)) for _, lead, index, _ in a]
    ins += [pl.BlockSpec((*lead, w), lambda i, j, index=index, column=column: (*index, column + j))
            for b, (_, w) in zip(bs, wides) for _, lead, index, column in b]
    return call(functools.partial(_outer, parts=parts, outs=len(bs), begun=len(begun), turned=turned), (end - begin, steps), ins,
                [((m, c), jnp.bfloat16, pl.BlockSpec((rows, w), lambda i, j: (i + begin, j))) for c, w in wides],
                [pltpu.VMEM((rows, depth), jnp.bfloat16)], [*begun, *(v[0] for v in a), *(v[0] for b in bs for v in b)],
                2 * depth * (end - begin) * rows * sum(c for c, _ in wides), aliases={i: i for i in range(len(begun))})


def normed(h):
    wide = h.astype(jnp.float32)
    scale = lax.rsqrt(jnp.mean(wide**2, -1, keepdims=True) + 1e-6)
    return bf(wide * scale)


def norm_back(h, d_out):
    wide, d_out = h.astype(jnp.float32), d_out.astype(jnp.float32)
    scale = lax.rsqrt(jnp.mean(wide**2, -1, keepdims=True) + 1e-6)
    return scale * d_out - wide * (scale**3 * jnp.mean(d_out * wide, -1, keepdims=True))


def solution(mesh):
    n = mesh.shape["tp"]
    parts = 2

    def gather(t):
        return lax.all_gather(t, "tp", axis=0, tiled=True)

    def scatter(t):
        return lax.psum_scatter(t, "tp", scatter_dimension=0, tiled=True)

    def after(t, *others):
        return lax.optimization_barrier((t, *others))[0]

    def step(x, dy, wq, wk, wv, wo, w_gate, w_up, w_down):
        x, dy = x[0], dy[0]
        tokens, d = x.shape
        size = tokens // parts
        every = range(parts)
        own = lambda t: [t[s * size : (s + 1) * size] for s in every]
        qs, ks, units = wq.shape[1], wk.shape[1], w_gate.shape[1]
        h, kv = qs // HEAD, ks // HEAD

        def stream(t, s):
            return t.reshape(n, parts, size, t.shape[-1]), (n, 1, size), (0, s, 0), 0

        half = HEAD // 2
        angle = jnp.arange(n * tokens, dtype=jnp.float32)[:, None] * THETA ** (-jnp.arange(half, dtype=jnp.float32) / half)
        cos, sin = jnp.cos(angle), jnp.sin(angle)
        cos, sin = jnp.concatenate([cos, cos], 1), jnp.concatenate([-sin, sin], 1)

        a, w_qkv, qkv = first(normed(x), wq, wk, wv, cos, sin, n)
        dys = [gather(after(t, a)) for t in own(dy)]
        heads, lse = look(qkv, h, kv)
        h1 = x + scatter(bf(_dot(heads, wo)))
        b = [gather(t) for t in own(normed(h1))]
        d_hidden = []
        for s in every:
            d_hidden.append(bf(_dot(dys[s], w_down, 1, 1)))
        hidden, b_turned, d_gate, d_up, d_h1, dhs = [], [], [], [], [], []
        for s in every:
            u, dg, du, bt = mlp(b[s], plain(d_hidden[s]), w_gate, w_up)
            term = mlp_back(after(dg, *d_h1), du, w_gate, w_up)
            by_b = after(scatter(term), *d_h1[-1:])
            d_h1.append(bf(own(dy)[s].astype(jnp.float32) + norm_back(own(h1)[s], by_b)))
            dhs.append(gather(d_h1[s]))
            hidden.append(plain(u)), b_turned.append(plain(bt)), d_gate.append(plain(dg)), d_up.append(plain(du))
        by_gate, = outer(b_turned, [d_gate], 512, 1, [(units, units)], turned=True)
        by_down = outer(hidden, [[plain(t) for t in dys]], 640, 1, [(d, d)], (0, 2), turned=True)
        d_heads, dqs, sums = [], [], ()
        for s in every:
            d_heads.append(back(dhs[s], wo, 256))
            dq, *sums = look_back(s, parts, n, qkv, h, kv, d_heads[s], heads, lse, cos, sin, sums)
            dqs.append(dq)
        dkv, = sums
        late = after(hidden[0][0], d_h1[-1])
        by_down, = outer([plain(late), *hidden[1:]], [[plain(t) for t in dys]], 640, 1, [(d, d)], (2, units // 640), by_down, turned=True)
        term = qkv_back(dqs, dkv, w_qkv, n)
        by_a = scatter(term)
        by_x = bf(jnp.concatenate(d_h1).astype(jnp.float32) + norm_back(x, by_a))
        by_up, = outer(b_turned, [d_up], 512, 1, [(units, units)], turned=True)
        by_wo, = outer([stream(heads, s) for s in every], [[plain(t) for t in dhs]], qs, 4, [(d, d // 4)])
        column = lambda c: [(*stream(dkv, s)[:3], c) for s in every]
        by_q, by_k, by_v = outer([stream(a, s) for s in every], [[plain(t) for t in dqs], column(0), column(1)], 512, 1, [(qs, qs), (ks, ks), (ks, ks)])
        return by_x[None], by_q, by_k, by_v, by_wo, by_gate, by_up, by_down

    states, by_columns, by_rows = P("dp", "tp", None), P(None, "tp"), P("tp", None)
    weights = (by_columns, by_columns, by_columns, by_rows, by_columns, by_columns, by_rows)
    own = tuple(P("dp", "tp") if spec == by_columns else P(("dp", "tp"), None) for spec in weights)
    return jax.shard_map(step, mesh=mesh, in_specs=(states, states, *weights), out_specs=(states, *own), check_vma=False)
```
